32 devices in a mesh: rep: 4 (over z), own: 8 (over y, x, core).
Axes of the slice: x: 2, y: 2, z: 4, core: 2. Of those that a mesh axis runs over, the one named last changes fastest.
Arguments:
- inputs: bfloat16 [8192, 8192], P(('rep', 'own')), may hold values from -6 to 6
- cotangent: bfloat16 [8192, 8192], P(('rep', 'own')), may hold values from -6 to 6
- gate: float32 [8192], P(('rep', 'own')), may hold values from 0.05 to 0.95
- down_weight: bfloat16 [8192, 256], P('rep'), may hold values from -0.0625 to 0.0625
- up_weight: bfloat16 [8192, 256], P('rep'), may hold values from -0.0625 to 0.0625
- mixing: bfloat16 [256, 256], replicated, may hold values from -0.375 to 0.375
- owner_table: int32 [8, 8], replicated, may hold values from -1 to 31, as said below
- left_factor: float32 [64, 256, 256], P('own'), as said below
- right_factor: float32 [64, 256, 256], P('own'), as said below
Outputs:
- preconditioned: float32 [16384, 256], P('own')
The draws below stay inside these ranges and needn't reach their ends.
Inputs may be any that keep to these rules, and one draw needn't show every extreme that they name: `owner_table`: each of the 32 block ids stands in exactly one slot; -1 marks an empty slot; some owner has all 8 slots filled. `left_factor`: every slot's matrix is symmetric positive definite. `right_factor`: every slot's matrix is symmetric positive definite.
All inputs are finite; a program needn't handle non-finite values.
Results may differ from the reference program's by a relative error of at most 0.0077.
Values may be sent and summed in bfloat16 or wider, within the bound.
No kernel may reach another device: no remote copies, remote signals or barrier semaphores. Data moves between devices by JAX's collectives and lax.ppermute only.
A program may use at most 128 MiB of HBM per device.

```python
import jax
import jax.numpy as jnp
from jax import lax

D = 8192
R = 256
ITERS = 5
B_DEV = 256
TOKENS = 8192
NBLK = 32
MOST = 8
N_OWN = 8


def draw_owner_table(key, part):
    slot_total = N_OWN * MOST
    first_key, second_key, third_key = jax.random.split(jax.random.fold_in(key, 7), 3)
    filled_owner = jax.random.randint(first_key, (), 0, N_OWN)
    shuffled = jax.random.permutation(second_key, slot_total).astype(jnp.int32)
    owner_ids = jnp.arange(slot_total, dtype=jnp.int32) // MOST
    priority = shuffled - slot_total * (owner_ids == filled_owner).astype(jnp.int32)
    ranked = jnp.argsort(priority, stable=True)
    block_order = jax.random.permutation(third_key, NBLK).astype(jnp.int32)
    contents = jnp.concatenate([block_order, jnp.full((slot_total - NBLK,), -1, jnp.int32)])
    assigned = jnp.zeros((slot_total,), jnp.int32).at[ranked].set(contents)
    return assigned.reshape(N_OWN, MOST)


def spd_factor(key):
    slot_total = N_OWN * MOST
    base_key = jax.random.fold_in(key, 0)
    samples = jax.random.normal(base_key, (slot_total, R, 2 * R), jnp.float32)
    gram = jnp.einsum('kij,klj->kil', samples, samples, precision=lax.Precision.HIGHEST)
    return gram * (0.01 / (2.0 * TOKENS))


def draw_left_factor(key, part):
    return spd_factor(jax.random.fold_in(key, 11))


def draw_right_factor(key, part):
    return spd_factor(jax.random.fold_in(key, 12))


def raised(entries, own_key, source, target, parts, factor):
    owner, partner = [(jnp.arange(entries.shape[axis_at]) // (entries.shape[axis_at] // parts)).reshape([-1 if axis == axis_at else 1 for axis in range(entries.ndim)]) for axis_at in (source, target)]
    chosen = jax.random.permutation(own_key, parts)[partner]
    strong = (owner == chosen) | (owner == (partner + parts // 2) % parts)
    return jnp.where(strong, factor * entries, entries)


def level_of(own_key, dims, cuts, least, high):
    loudness, own = 1.0, jax.random.fold_in(own_key, 6)
    for dim, parts in cuts:
        heights = jnp.exp(jax.random.uniform(jax.random.fold_in(own, dim), (parts,), jnp.float32, least / len(cuts), high / len(cuts)))
        loudness = loudness * jnp.repeat(heights, dims[dim] // parts).reshape([-1 if axis == dim else 1 for axis in range(len(dims))])
    return loudness


def noise(stream_key, shape, spread, most, cuts=(), kind=jnp.bfloat16):
    drawn = jax.random.normal(stream_key, shape, jnp.float32) * spread
    if len(cuts) > 0:
        drawn = level_of(stream_key, shape, cuts, -0.22, 0.18) * drawn
    return jnp.clip(drawn, min=-most, max=most).astype(kind)


def noise_with(own_key, dims, deviation, limit, cuts, heavy, kind=jnp.bfloat16):
    values = deviation * jax.random.normal(own_key, dims, jnp.float32)
    if cuts:
        values = values * level_of(own_key, dims, cuts, -0.22, 0.18)
    return jnp.clip(raised(values, jax.random.fold_in(own_key, 3), *heavy), -limit, limit).astype(kind)


def setup_inputs(seed: int = 0) -> dict:
    seeds = jax.random.split(jax.random.key(seed), 10)
    return {
        "inputs": noise_with(seeds[0], (TOKENS, D), 1.0, 6.0, ((0, 32),), (0, 1, 32, 2.75)),
        "cotangent": noise(seeds[1], (TOKENS, D), 1.0, 6.0, ((0, 32),)),
        "gate": jnp.clip(0.05 + 0.9 * jax.random.uniform(seeds[2], (TOKENS,), jnp.float32) ** level_of(seeds[2], (TOKENS,), ((0, 32),), -0.2, 0.2), 0.05, 0.95),
        "down_weight": noise(seeds[3], (D, R), D ** -0.5, 0.0625, ((0, 4),)),
        "up_weight": noise(seeds[4], (D, R), D ** -0.5, 0.0625, ((0, 4),)),
        "mixing": noise(seeds[5], (R, R), R ** -0.5, 0.375),
        "owner_table": draw_owner_table(jax.random.fold_in(seeds[9], 71), 0),
        "left_factor": draw_left_factor(jax.random.fold_in(seeds[9], 71), 0),
        "right_factor": draw_right_factor(jax.random.fold_in(seeds[9], 71), 0),
    }


BETA = 0.95
EPS = 1e-06

def batched(left, right):
    return jnp.einsum('kij,kjl->kil', left, right, precision=lax.Precision.HIGHEST)

def inverse_root(matrices):
    width = matrices.shape[-1]
    identity = jnp.eye(width, dtype=jnp.float32)
    shifted = matrices + EPS * identity
    norm_size = jnp.sqrt(lax.optimization_barrier(jnp.sum(shifted * shifted, axis=(1, 2))))
    result = jnp.broadcast_to(identity, shifted.shape) * (norm_size ** (-0.25))[:, None, None]
    normed = shifted / norm_size[:, None, None]
    for sweep in range(ITERS):
        factor = (5.0 * identity - normed) / 4.0
        result = batched(result, factor)
        square = batched(factor, factor)
        normed = batched(batched(square, square), normed)
    return result

def backward_signal(rows, tangent, gate_rows, down_weight, up_weight, mixing):
    lifted = (gate_rows[:, None] * rows.astype(jnp.float32) * tangent.astype(jnp.float32)).astype(jnp.bfloat16)
    projected = jnp.dot(rows, down_weight, preferred_element_type=jnp.float32)
    back_proj = jnp.dot(lifted, up_weight, preferred_element_type=jnp.float32)
    inner_act = jnp.tanh(projected).astype(jnp.bfloat16)
    outer_act = jnp.tanh(jnp.dot(inner_act, mixing, preferred_element_type=jnp.float32))
    outer_slope = (back_proj * (1.0 - outer_act * outer_act)).astype(jnp.bfloat16)
    through = lax.dot_general(outer_slope, mixing, (((1,), (1,)), ((), ())), preferred_element_type=jnp.float32)
    inner_wide = inner_act.astype(jnp.float32)
    return (through * (1.0 - inner_wide * inner_wide)).astype(jnp.bfloat16)

def reference(inputs, cotangent, gate, down_weight, up_weight, mixing, owner_table, left_factor, right_factor):
    group_count = inputs.shape[0] // B_DEV

    def accumulate(summed, minibatch):
        rows, tangent, gate_rows = minibatch
        signal = backward_signal(rows, tangent, gate_rows, down_weight, up_weight, mixing)
        return (summed + lax.dot_general(rows, signal, (((0,), (0,)), ((), ())), preferred_element_type=jnp.float32), None)
    start_sum = jnp.zeros((D, R), jnp.float32)
    gradient, _ = lax.scan(accumulate, start_sum, (inputs.reshape(group_count, B_DEV, D), cotangent.reshape(group_count, B_DEV, D), gate.reshape(group_count, B_DEV)))
    gradient = gradient / TOKENS
    table_flat = owner_table.reshape(-1)
    filled_slots = (table_flat >= 0)[:, None, None]
    blocks = gradient.reshape(NBLK, R, R)
    gradients = jnp.where(filled_slots, blocks[jnp.maximum(table_flat, 0).astype(jnp.int32)], 0.0)
    flipped = jnp.swapaxes(gradients, 1, 2)
    left_new = BETA * left_factor + (1.0 - BETA) * batched(gradients, flipped)
    right_new = BETA * right_factor + (1.0 - BETA) * batched(flipped, gradients)
    slot_total = N_OWN * MOST
    left_root = inverse_root(left_new)
    right_root = inverse_root(right_new)
    preconditioned = batched(batched(left_root, gradients), right_root)
    return jnp.where(filled_slots, preconditioned, 0.0).reshape(slot_total * R, R)
```

```python
import functools

import jax
import jax.numpy as jnp
from jax import lax
from jax.experimental import pallas as pl
from jax.experimental.pallas import tpu as pltpu
from jax.sharding import PartitionSpec as P

ITERS = 5
BETA = 0.95
EPS = 1e-06


F32 = jnp.float32
BF16 = jnp.bfloat16

CORE, XBIT, YBIT = 1, 2, 4


def own_swap(value, mask):
    size = lax.axis_size("own")
    return lax.ppermute(value, "own", [(i, i ^ mask) for i in range(size)])


def rep_swap(value, mask):
    size = lax.axis_size("rep")
    return lax.ppermute(value, "rep", [(i, i ^ mask) for i in range(size)])


def mm(left, right, contract=((1,), (0,))):
    return lax.dot_general(left, right, (contract, ((), ())), preferred_element_type=F32)


def mm_bf(left, right, contract=((1,), (0,))):
    return mm(left.astype(BF16), right.astype(BF16), contract)


def split(value):
    high = value.astype(BF16)
    return high, (value - high.astype(F32)).astype(BF16)


def batched(left, right):
    return jnp.einsum("kij,kjl->kil", left, right, precision=lax.Precision.HIGHEST)


def inverse_root(matrices):
    width = matrices.shape[-1]
    identity = jnp.eye(width, dtype=jnp.float32)
    shifted = matrices + EPS * identity
    norm_size = jnp.sqrt(jnp.sum(shifted * shifted, axis=(1, 2)))
    result = jnp.broadcast_to(identity, shifted.shape) * (norm_size ** (-0.25))[:, None, None]
    normed = shifted / norm_size[:, None, None]
    for sweep in range(ITERS):
        factor = (5.0 * identity - normed) / 4.0
        result = batched(result, factor)
        square = batched(factor, factor)
        normed = batched(batched(square, square), normed)
    return result


def general_shards(
    inputs, cotangent, gate, down_weight, up_weight, mixing, owner_table, left_factor, right_factor
):
    R = down_weight.shape[1]
    token_total = inputs.shape[0] * lax.axis_size("rep") * lax.axis_size("own")
    slot_count = left_factor.shape[0]
    lifted = (gate[:, None] * inputs.astype(jnp.float32) * cotangent.astype(jnp.float32)).astype(
        jnp.bfloat16
    )
    columns = inputs
    projected = jnp.dot(
        columns,
        lax.all_gather(down_weight, "rep", axis=0, tiled=True),
        preferred_element_type=jnp.float32,
    )
    back_proj = jnp.dot(
        lifted,
        lax.all_gather(up_weight, "rep", axis=0, tiled=True),
        preferred_element_type=jnp.float32,
    )
    inner_act = jnp.tanh(projected).astype(jnp.bfloat16)
    outer_act = jnp.tanh(jnp.dot(inner_act, mixing, preferred_element_type=jnp.float32))
    outer_slope = (back_proj * (1.0 - outer_act * outer_act)).astype(jnp.bfloat16)
    through = lax.dot_general(
        outer_slope, mixing, (((1,), (1,)), ((), ())), preferred_element_type=jnp.float32
    )
    inner_wide = inner_act.astype(jnp.float32)
    signal = (through * (1.0 - inner_wide * inner_wide)).astype(jnp.bfloat16)
    columns = inputs
    shard = lax.psum_scatter(
        lax.dot_general(
            columns, signal, (((0,), (0,)), ((), ())), preferred_element_type=jnp.float32
        )
        / token_total,
        "own",
        scatter_dimension=0,
        tiled=True,
    )
    shard = lax.psum(shard, "rep")
    my_blocks = lax.dynamic_index_in_dim(owner_table, lax.axis_index("own"), 0, keepdims=False)
    wanted = (
        jnp.maximum(my_blocks, 0)[:, None] * R + jnp.arange(R, dtype=jnp.int32)[None, :]
    ).reshape(-1)
    shard_rows = lax.all_gather(shard, "own", axis=0, tiled=True)
    row_total = shard_rows.shape[0]
    inside = (wanted >= 0) & (wanted < row_total)
    selected = jnp.take(shard_rows, jnp.clip(wanted, 0, row_total - 1), axis=0)
    owned = jnp.where(inside[:, None], selected, jnp.zeros((slot_count * R, R), jnp.float32))
    my_row = lax.dynamic_index_in_dim(owner_table, lax.axis_index("own"), 0, keepdims=False)
    filled_slots = (my_row >= 0)[:, None, None]
    gradients = jnp.where(filled_slots, owned.reshape(slot_count, R, R), 0.0)
    flipped = jnp.swapaxes(gradients, 1, 2)
    left_new = BETA * left_factor + (1.0 - BETA) * batched(gradients, flipped)
    right_new = BETA * right_factor + (1.0 - BETA) * batched(flipped, gradients)
    factors = jnp.concatenate([left_new, right_new], axis=0)
    inverse_roots = inverse_root(factors)
    preconditioned = batched(
        batched(inverse_roots[:slot_count], gradients), inverse_roots[slot_count:]
    )
    return jnp.where(filled_slots, preconditioned, 0.0).reshape(slot_count * R, R)


def tables_kernel(where_ref, table_ref, cols_ref, info_ref, sel_ref, block_ref, seen_ref, *, reps):
    owners, slots = table_ref.shape
    each = info_ref.shape[0] // 3
    rep_at, own_at = where_ref[0], where_ref[1]
    for i in range(3 * each):
        info_ref[i] = 0
    for i in range(reps):
        seen_ref[i] = 0

    def visit(at, rank):
        owner, slot = at // slots, at % slots
        block = table_ref[owner, slot]
        filled = block >= 0
        mine = owner == own_at
        home = rank % reps

        @pl.when(filled)
        def _():
            block_ref[rank] = block

        @pl.when(filled & mine)
        def _():
            turn = seen_ref[home]
            seen_ref[home] = turn + 1
            mask = jnp.bitwise_xor(rep_at, home)
            at_end = (rep_at == 0) | (rep_at == reps - 1)
            source = jnp.where((mask == 3) & at_end, 4, mask)
            sel_ref[slot] = source * each + turn

            @pl.when(home == rep_at)
            def _():
                info_ref[turn] = jnp.bitwise_xor(own_at, rank // reps)
                info_ref[each + turn] = slot
                info_ref[2 * each + turn] = 1

        @pl.when(mine & (block < 0))
        def _():
            sel_ref[slot] = -1

        return rank + filled.astype(jnp.int32)

    lax.fori_loop(0, owners * slots, visit, jnp.int32(0))
    for i in range(cols_ref.shape[0]):
        device = jnp.bitwise_xor(own_at, (i // reps) * 2)
        cols_ref[i] = block_ref[reps * device + jnp.bitwise_xor(rep_at, i % reps)]


def tables(where, owner_table, reps):
    owners, slots = owner_table.shape
    each = -(-slots // reps)
    smem = pl.BlockSpec(memory_space=pltpu.SMEM)
    shape = lambda n: jax.ShapeDtypeStruct((n,), jnp.int32)
    return pl.pallas_call(
        functools.partial(tables_kernel, reps=reps),
        out_shape=[shape(owners // 2 * reps), shape(3 * each), shape(slots)],
        in_specs=[smem, smem],
        out_specs=[smem, smem, smem],
        scratch_shapes=[pltpu.SMEM((owners * reps,), jnp.int32), pltpu.SMEM((reps,), jnp.int32)],
        name="tables",
    )(where, owner_table)


def plane_kernel(where_ref, *refs, first, sides):
    x_ref, twin_x_ref, cot_ref, twin_cot_ref, gate_ref, twin_gate_ref = refs[:6]
    pieces, out_refs = refs[6 : 6 + sides], refs[-2:]
    step = pl.program_id(0)
    x, twin_x = x_ref[...], twin_x_ref[...]
    rows, chunk = x.shape
    lift = lambda g, a, b: (g[...] * a.astype(F32) * b[...].astype(F32)).astype(BF16)
    wide = jnp.concatenate([x, twin_x], axis=0)
    lifted = jnp.concatenate([lift(gate_ref, x, cot_ref), lift(twin_gate_ref, twin_x, twin_cot_ref)], axis=0)

    def add(down, up, starts):
        for side, part in enumerate((mm(wide, down), mm(lifted, up))):
            for out, start, half in zip(out_refs, starts, (part[:rows], part[rows:])):
                if start is None:
                    out[side] = half
                else:
                    out[side] = start[side] + half

    if first:
        down, up = pieces[0][...], pieces[1][...]

        @pl.when(step == 0)
        def _():
            add(down, up, (None, None))

        @pl.when(step > 0)
        def _():
            add(down, up, out_refs)

    else:
        acc_refs = refs[6 + sides : 8 + sides]
        for at, piece in enumerate(pieces):

            @pl.when(step == at)
            def _():
                add(piece[:chunk, :], piece[chunk:, :], out_refs if at else acc_refs)


def plane(where, mask, data, pieces, acc=None):
    x, twin_x, cot, twin_cot, gate, twin_gate = data
    rows = x.shape[0]
    owns = lax.axis_size("own")
    steps = owns // 2
    rank = pieces[0].shape[1]
    chunk = x.shape[1] // (owns * lax.axis_size("rep"))
    whole = lambda a: pl.BlockSpec(a.shape, lambda i, w: (0,) * a.ndim)
    column = pl.BlockSpec(
        (rows, chunk),
        lambda i, w: (0, jnp.bitwise_xor(w[0], mask) * owns + jnp.bitwise_xor(w[1], 2 * i)),
    )
    first = acc is None
    if first:
        piece_specs = [pl.BlockSpec((chunk, rank), lambda i, w: (jnp.bitwise_xor(w[1], 2 * i), 0))] * 2
        acc = []
    else:
        piece_specs = [whole(a) for a in pieces]
    out = jax.ShapeDtypeStruct((2, rows, rank), F32)
    return pl.pallas_call(
        functools.partial(plane_kernel, first=first, sides=len(pieces)),
        out_shape=[out, out],
        grid_spec=pltpu.PrefetchScalarGridSpec(
            num_scalar_prefetch=1,
            grid=(steps,),
            in_specs=[column] * 4 + [whole(gate)] * 2 + piece_specs + [whole(a) for a in acc],
            out_specs=[whole(out), whole(out)],
        ),
        cost_estimate=pl.CostEstimate(
            flops=steps * 8 * rows * chunk * rank, bytes_accessed=steps * 8 * rows * chunk, transcendentals=0
        ),
        name=f"plane_{mask}",
    )(where, x, twin_x, cot, twin_cot, gate, twin_gate, *pieces, *acc)


def signal_kernel(mine_ref, got_ref, mixing_ref, signal_ref):
    projected = mine_ref[0] + got_ref[0]
    back_proj = mine_ref[1] + got_ref[1]
    mixing = mixing_ref[...]
    inner_act = jnp.tanh(projected).astype(BF16)
    outer_act = jnp.tanh(mm(inner_act, mixing))
    outer_slope = (back_proj * (1.0 - outer_act * outer_act)).astype(BF16)
    through = mm(outer_slope, mixing, ((1,), (1,)))
    inner_wide = inner_act.astype(F32)
    signal = through * (1.0 - inner_wide * inner_wide)
    signal_ref[...] = signal.T.astype(BF16)


def signal_of(mine, got, mixing):
    rows, rank = mine.shape[1:]
    return pl.pallas_call(
        signal_kernel,
        out_shape=jax.ShapeDtypeStruct((rank, rows), BF16),
        name="signal",
    )(mine, got, mixing)


def gradient_kernel(cols_ref, mine_ref, twin_ref, x_ref, twin_x_ref, out_ref):
    signals = jnp.concatenate([mine_ref[...], twin_ref[...]], axis=1)
    columns = jnp.concatenate([x_ref[...], twin_x_ref[...]], axis=0)
    out_ref[0] = mm(signals, columns).astype(out_ref.dtype)


def gradient_part(cols, mine, twin, x, twin_x, place, dtype, name):
    rank, rows = mine.shape
    column = pl.BlockSpec((rows, rank), lambda h, l, c: (0, c[place(h, l)]))
    whole = pl.BlockSpec((rank, rows), lambda h, l, c: (0, 0))
    return pl.pallas_call(
        gradient_kernel,
        out_shape=jax.ShapeDtypeStruct((4, rank, rank), dtype),
        grid_spec=pltpu.PrefetchScalarGridSpec(
            num_scalar_prefetch=1,
            grid=(2, 2),
            in_specs=[whole, whole, column, column],
            out_specs=pl.BlockSpec((1, rank, rank), lambda h, l, c: (2 * h + l, 0, 0)),
        ),
        cost_estimate=pl.CostEstimate(
            flops=16 * rows * rank * rank, bytes_accessed=16 * rows * rank, transcendentals=0
        ),
        name=name,
    )(cols, mine, twin, x, twin_x)


def root_kernel(info_ref, *rest, slots, tokens):
    blocks = rest[:8]
    lefts, rights = rest[8 : 8 + slots], rest[8 + slots : 8 + 2 * slots]
    out_ref, stack_ref = rest[-2], rest[-1]
    for at, ref in enumerate(blocks):
        stack_ref[at] = ref[...]
    width = stack_ref.shape[1]
    row = lax.broadcasted_iota(jnp.int32, (width, width), 0)
    col = lax.broadcasted_iota(jnp.int32, (width, width), 1)
    ridge = jnp.where(row == col, jnp.float32(EPS), jnp.float32(0.0))
    flips, normed, scales = [], [], []
    for j in range(slots):
        flip = stack_ref[info_ref[j]]
        flips.append(flip)
        left = BETA * lefts[j][0] + (1.0 - BETA) * mm(flip, flip, ((0,), (0,)))
        right = BETA * rights[j][0] + (1.0 - BETA) * mm(flip, flip, ((1,), (1,)))
        for matrix in (left, right):
            shifted = matrix + ridge
            size = jnp.sqrt(jnp.sum(shifted * shifted, keepdims=True))
            normed.append(shifted / size)
            scales.append(lax.rsqrt(jnp.sqrt(size)))
    roots = [None] * len(normed)
    for sweep in range(ITERS):
        for at in range(len(normed)):
            n = normed[at] * 0.2
            n_low = n.astype(BF16)
            if roots[at] is None:
                roots[at] = -n
            else:
                roots[at] = roots[at] - n - mm(roots[at].astype(BF16), n_low)
            if sweep + 1 < ITERS:
                e = 2.0 * n - mm(n_low, n_low)
                e_low = e.astype(BF16)
                q = 2.0 * e - mm(e_low, e_low)
                normed[at] = (1.25**4) * (normed[at] - mm_bf(q, normed[at]))
    for j in range(slots):
        left, right = roots[2 * j], roots[2 * j + 1]
        flip = flips[j]
        left_high, left_low = split(left)
        half = flip.astype(F32).T + (
            mm(left_high, flip, ((1,), (1,))) + mm(left_low, flip, ((1,), (1,)))
        )
        half_high, half_low = split(half)
        right_high, right_low = split(right)
        full = half + (mm(half_high, right_high) + (mm(half_low, right_high) + mm(half_high, right_low)))
        scale = scales[2 * j] * scales[2 * j + 1] * (1.25 ** (2 * ITERS))
        full = full * scale
        out_ref[j] = jnp.where(info_ref[2 * slots + j] > 0, full, 0.0).astype(out_ref.dtype)


def roots(info, blocks, left_factor, right_factor, slots, tokens):
    rank = left_factor.shape[1]
    block_spec = pl.BlockSpec((rank, rank), lambda i, n: (0, 0))
    factor_spec = lambda j: pl.BlockSpec((1, rank, rank), lambda i, n: (n[slots + j], 0, 0))
    return pl.pallas_call(
        functools.partial(root_kernel, slots=slots, tokens=tokens),
        out_shape=jax.ShapeDtypeStruct((slots, rank, rank), BF16),
        grid_spec=pltpu.PrefetchScalarGridSpec(
            num_scalar_prefetch=1,
            grid=(1,),
            in_specs=[block_spec] * 8
            + [factor_spec(j) for j in range(slots)]
            + [factor_spec(j) for j in range(slots)],
            out_specs=pl.BlockSpec((slots, rank, rank), lambda i, n: (0, 0, 0)),
            scratch_shapes=[pltpu.VMEM((8, rank, rank), BF16)],
        ),
        name="roots",
    )(info, *blocks, *([left_factor] * slots), *([right_factor] * slots))


def spread_kernel(sel_ref, *rest, slots):
    sources, out_ref = rest[:-1], rest[-1]
    rank = sources[0].shape[1]
    for at in range(out_ref.shape[0] // rank):
        rows = pl.ds(at * rank, rank)
        pick = sel_ref[pl.program_id(0) * (out_ref.shape[0] // rank) + at]
        for k, source in enumerate(sources):

            @pl.when((pick >= k * slots) & (pick < (k + 1) * slots))
            def _():
                out_ref[rows, :] = source[pick - k * slots].astype(F32)

        @pl.when(pick < 0)
        def _():
            out_ref[rows, :] = jnp.zeros((rank, rank), F32)


def spread(sel, sources):
    slots, rank, _ = sources[0].shape
    count = sel.shape[0]
    steps = 2
    return pl.pallas_call(
        functools.partial(spread_kernel, slots=slots),
        out_shape=jax.ShapeDtypeStruct((count * rank, rank), F32),
        grid_spec=pltpu.PrefetchScalarGridSpec(
            num_scalar_prefetch=1,
            grid=(steps,),
            in_specs=[pl.BlockSpec((slots, rank, rank), lambda i, n: (0, 0, 0))] * len(sources),
            out_specs=pl.BlockSpec((count // steps * rank, rank), lambda i, n: (i, 0)),
        ),
        name="spread",
    )(sel, *sources)


def fast_shards(
    inputs, cotangent, gate, down_weight, up_weight, mixing, owner_table, left_factor, right_factor
):
    reps, owns = lax.axis_size("rep"), lax.axis_size("own")
    rows = inputs.shape[0]
    token_total = rows * reps * owns
    chunk = down_weight.shape[0] // owns
    each = -(-owner_table.shape[1] // reps)
    rep_at, own_at = lax.axis_index("rep"), lax.axis_index("own")
    where = jnp.stack([rep_at, own_at]).astype(jnp.int32)

    cut = lambda w: lax.dynamic_slice_in_dim(w, own_at * chunk, chunk, 0)
    piece = jnp.concatenate([cut(down_weight), cut(up_weight)], axis=0)
    planes = []
    for k in range(1, reps):
        mine = rep_swap(piece, k)
        across_x, across_y = own_swap(mine, XBIT), own_swap(mine, YBIT)
        if k == 1:
            corner = own_swap(across_y, XBIT)
        elif k == 2:
            corner = own_swap(across_x, YBIT)
        else:
            corner = own_swap(mine, XBIT + YBIT)
        planes.append([mine, across_x, across_y, corner])

    column_gate = gate[:, None]
    twin_x, twin_cot = own_swap(inputs, CORE), own_swap(cotangent, CORE)
    twin_gate = own_swap(gate, CORE)[:, None]
    cols, info, sel = tables(where, owner_table, reps)
    data = (inputs, twin_x, cotangent, twin_cot, column_gate, twin_gate)
    acc = plane(where, 0, data, [down_weight, up_weight])
    for k in range(1, reps):
        acc = plane(where, k, data, planes[k - 1], acc)
    signal = signal_of(acc[0], own_swap(acc[1], CORE), mixing)
    twin_signal = own_swap(signal, CORE)

    def part(place, dtype, name):
        return gradient_part(cols, signal, twin_signal, inputs, twin_x, place, dtype, name)

    top_place = lambda b: lambda h, l: (2 * h + b) * reps + l
    low_place = lambda a: lambda h, l: (2 * a + h) * reps + 2 + l
    got_top = own_swap(part(top_place(1), BF16, "top_sent"), XBIT)
    got_low = own_swap(part(low_place(1), BF16, "low_sent"), YBIT)
    top, low = part(top_place(0), F32, "top_kept"), part(low_place(0), F32, "low_kept")
    got_top2 = own_swap((top[2:] + got_top[2:].astype(F32)).astype(BF16), YBIT)
    got_low2 = own_swap((low[2:] + got_low[2:].astype(F32)).astype(BF16), XBIT)
    total = lambda kept, got, got2, k: kept[k] + got[k].astype(F32) + got2[k].astype(F32)
    got = [rep_swap(total(low, got_low, got_low2, k - 2).astype(BF16), k) for k in (2, 3)]
    got.append(rep_swap(total(top, got_top, got_top2, 1).astype(BF16), 1))
    block = total(top, got_top, got_top2, 0)
    for value in got:
        block = block + value.astype(F32)
    block = (block / token_total).astype(BF16)

    ring = [block] + [own_swap(block, mask) for mask in (XBIT, YBIT, XBIT + YBIT)]
    twins = [own_swap(value, CORE) for value in ring]
    blocks = [value for pair in zip(ring, twins) for value in pair]
    result = roots(info, blocks, left_factor, right_factor, each, token_total)
    across = rep_swap(result, 2)
    beside = rep_swap(result, 1)
    middle = lax.ppermute(result, "rep", [(0, 0), (1, 2), (2, 1), (3, 3)])
    passed_on = rep_swap(across, 1)
    return spread(sel, [result, beside, across, middle, passed_on])


def solution(mesh):
    in_specs = (
        P(("rep", "own"), None),
        P(("rep", "own"), None),
        P(("rep", "own")),
        P("rep", None),
        P("rep", None),
        P(),
        P(),
        P("own", None, None),
        P("own", None, None),
    )
    out_specs = P("own", None)

    def whole(inputs, cotangent, gate, down, up, mixing, table, left, right):
        reps, owns = mesh.shape["rep"], mesh.shape["own"]
        rows, width, rank = inputs.shape[0] // (reps * owns), inputs.shape[1], down.shape[1]
        fits = owns == 8 and reps == 4 and width == rank * reps * owns and rank == 256
        body = fast_shards if fits and rows == 256 else general_shards
        return jax.shard_map(
            body, mesh=mesh, in_specs=in_specs, out_specs=out_specs, check_vma=False
        )(inputs, cotangent, gate, down, up, mixing, table, left, right)

    return whole
```
